32 devices in a mesh: tok: 8 (over z, y), voc: 4 (over x, core).
Axes of the slice: x: 2, y: 2, z: 4, core: 2. Of those that a mesh axis runs over, the one named last changes fastest.
Arguments:
- hidden: bfloat16 [96, 4096], P(('tok', 'voc'))
- head_weight: bfloat16 [4096, 16032], P(None, ('tok', 'voc'))
- actions: int32 [96], P(('tok', 'voc')), may hold values from 0 to 16031
- old_logp: bfloat16 [96], P(('tok', 'voc')), may hold values from -80 to 1
- advantage: bfloat16 [96], P(('tok', 'voc')), may hold values from -4 to 4
- loss_mask: int32 [96], P(('tok', 'voc')), may hold values 0 or 1
Outputs:
- grad_weight: bfloat16 [4096, 16032], P(None, ('tok', 'voc'))
- grad_hidden: float32 [96, 4096], P(('tok', 'voc'))
The draws below stay inside these ranges and needn't reach their ends.
All inputs are finite; a program needn't handle non-finite values. No bound on the sum of `loss_mask` on one device may be relied on, other than what follows from the above.
Results may differ from the reference program's by a relative error of at most 0.0047.
Values may be sent and summed in bfloat16 or wider, within the bound.
A program may use at most 128 MiB of HBM per device.

```python
import jax
import jax.numpy as jnp
from jax import lax

D = 4096
VOCAB = 16032
TOKENS = 96


def unscaled_columns(key):
    wkey = jax.random.fold_in(key, 11)
    columns = jnp.arange(VOCAB)
    return jax.vmap(lambda c: jax.random.normal(jax.random.fold_in(wkey, c), (D,), jnp.float32))(columns)


def head_from(columns):
    return (jnp.transpose(columns) * (3.0 / jnp.sqrt(jnp.float32(D)))).astype(jnp.bfloat16)


def sampled_ids(key):
    return jax.random.randint(jax.random.fold_in(key, 13), (TOKENS,), 0, VOCAB).astype(jnp.int32)


def make_hidden(key, columns, chosen):
    hkey = jax.random.fold_in(key, 17)
    values = jax.random.normal(hkey, (TOKENS, D), jnp.float32)
    return values.astype(jnp.bfloat16)


def draw_head_weight(key, part):
    return head_from(unscaled_columns(key))


def draw_actions(key, part):
    return sampled_ids(key)


def draw_hidden(key, part):
    columns = unscaled_columns(key)
    return make_hidden(key, columns, sampled_ids(key))


def draw_old_logp(key, part):
    columns = unscaled_columns(key)
    chosen = sampled_ids(key)
    states = make_hidden(key, columns, chosen)
    logits = jnp.dot(states, head_from(columns), preferred_element_type=jnp.float32)
    top = jnp.max(logits, axis=1)
    lse = top + jnp.log(jnp.sum(jnp.exp(logits - top[:, None]), axis=1))
    target = jnp.take_along_axis(logits, chosen[:, None], axis=1)[:, 0]
    noise = jax.random.uniform(jax.random.fold_in(key, 19), (TOKENS,), jnp.float32, -0.5, 0.5)
    return jnp.clip(target - lse + noise, -80.0, 1.0).astype(jnp.bfloat16)


def with_ends(result, stream_key, least, top_value):
    extent = result.shape
    index_at = [jax.random.randint(jax.random.fold_in(stream_key, axis), (), 0, extent[axis]) for axis in range(len(extent))]
    result = result.at[tuple(index_at)].set(least)
    longest = extent.index(max(extent))
    index_at[longest] = (index_at[longest] + 1) % extent[longest]
    return result.at[tuple(index_at)].set(top_value)


def block_levels(key, dims, cuts, least, high):
    def one(axis_at, parts):
        heights = jax.random.uniform(jax.random.fold_in(jax.random.fold_in(key, 6), axis_at), (parts,), jnp.float32, least / len(cuts), high / len(cuts))
        return jnp.repeat(jnp.exp(heights), dims[axis_at] // parts).reshape((-1,) + (1,) * (len(dims) - axis_at - 1))

    loudness = one(*cuts[0])
    for cut in cuts[1:]:
        loudness = loudness * one(*cut)
    return loudness


def scatter_about(stream_key, dims, spread, most, split=(), held_as=jnp.bfloat16):
    factor_of = block_levels(stream_key, dims, split, -0.22, 0.18) if split else 1.0
    entries = jax.random.normal(stream_key, dims, jnp.float32) * spread * factor_of
    return jnp.minimum(jnp.maximum(entries, -most), most).astype(held_as)


def setup_inputs(seed: int = 0) -> dict:
    key_list = jax.random.split(jax.random.key(seed), 7)
    return {
        "hidden": draw_hidden(jax.random.fold_in(key_list[6], 71), 0),
        "head_weight": draw_head_weight(jax.random.fold_in(key_list[6], 71), 0),
        "actions": draw_actions(jax.random.fold_in(key_list[6], 71), 0),
        "old_logp": draw_old_logp(jax.random.fold_in(key_list[6], 71), 0),
        "advantage": scatter_about(key_list[4], (TOKENS,), 1.0, 4.0, ((0, 32),)),
        "loss_mask": with_ends((jax.random.randint(key_list[5], (TOKENS,), 0, 4) < 3).astype(jnp.int32), jax.random.fold_in(key_list[5], 1), 0, 1),
    }


def reference(hidden, head_weight, actions, old_logp, advantage, loss_mask):
    logits = jnp.dot(hidden, head_weight, preferred_element_type=jnp.float32)
    top = jnp.max(logits, axis=1)
    shifted = jnp.exp(logits - top[:, None])
    sumexp = jnp.sum(shifted, axis=1)
    moment = jnp.sum(shifted * logits, axis=1)
    target = jnp.take_along_axis(logits, actions[:, None].astype(jnp.int32), axis=1)[:, 0]
    lse = top + jnp.log(sumexp)
    mean_logit = moment / sumexp
    logp = target - lse
    advant = advantage.astype(jnp.float32)
    ratio = jnp.exp(logp - old_logp.astype(jnp.float32))
    clipped = ((advant > 0.0) & (ratio > 1.2)) | ((advant < 0.0) & (ratio < 0.8))
    active = jnp.where(clipped, 0.0, 1.0).astype(jnp.float32)
    weights = loss_mask.astype(jnp.float32)
    policy = -advant * ratio * active * weights
    probability = jnp.exp(logits - lse[:, None])
    columns = lax.broadcasted_iota(jnp.int32, logits.shape, 1)
    onehot = (columns == actions[:, None].astype(jnp.int32)).astype(jnp.float32)
    dlogits = policy[:, None] * (onehot - probability) + 0.05 * weights[:, None] * probability * (logits - mean_logit[:, None])
    dlogits = dlogits.astype(jnp.bfloat16)
    grad_weight = lax.dot_general(hidden, dlogits, (((0,), (0,)), ((), ())), preferred_element_type=jnp.float32).astype(jnp.bfloat16)
    grad_hidden = lax.dot_general(dlogits, head_weight, (((1,), (1,)), ((), ())), preferred_element_type=jnp.float32)
    return grad_weight, grad_hidden
```

```python
import functools

import jax
import jax.numpy as jnp
from jax import lax
from jax.experimental import pallas as pl
from jax.experimental.pallas import tpu as pltpu
from jax.sharding import PartitionSpec as P

MESH = pl.DeviceIdType.MESH
F32, BF16 = jnp.float32, jnp.bfloat16
LANES = 128


def step_of(size, most):
    best = LANES
    for k in range(LANES, most + 1, LANES):
        if size % k == 0:
            best = k
    return best


def kernel(dims, real, hx_ref, wt_hbm, gh_ref, dt_ref, gall_ref,
           wt, slab, stage, g, own, stats, logit, pb, rc, ra1, ra2, rb1, rb2, q, rz,
           w_sem, zs, zr, s1, r1, s2, r2, cs, cr, ss, sr, ks, kr, t1s, t1r, t2s, t2r, us, ur):
    Z, Y, X, C = dims
    n = Z * Y * X * C
    V = X * C
    rp = hx_ref.shape[0]
    width, D = wt.shape
    R = Z * rp
    T = n * rp
    tok, voc = lax.axis_index("tok"), lax.axis_index("voc")
    z, y = tok // Y, lax.rem(tok, Y)
    x, c = voc // C, lax.rem(voc, C)
    me = tok * V + voc

    load = pltpu.make_async_copy(wt_hbm, wt, w_sem)
    load.start()

    def device(zz, yy, xx, cc):
        return (zz * Y + yy, xx * C + cc)

    def at_offset(k):
        other = lax.rem(me + k, n)
        return (other // V, lax.rem(other, V))

    barrier = pltpu.get_barrier_semaphore()

    def greet(k, carry):
        pl.semaphore_signal(barrier, inc=1, device_id=at_offset(k), device_id_type=MESH)
        return carry

    lax.fori_loop(1, n, greet, 0)
    pl.semaphore_wait(barrier, n - 1)

    started = []

    def send(src, dst, ssem, rsem, dev):
        copy = pltpu.make_async_remote_copy(
            src_ref=src, dst_ref=dst, send_sem=ssem, recv_sem=rsem, device_id=dev, device_id_type=MESH
        )
        copy.start()
        started.append(copy)
        return copy

    line = [
        send(hx_ref, slab.at[z], zs.at[k], zr.at[k], device(lax.rem(z + k, Z), y, x, c))
        for k in range(1, Z)
    ]
    slab[z] = hx_ref[...]
    for copy in line:
        copy.wait_recv()
    for zi in range(Z):
        stage[zi * rp:(zi + 1) * rp, :] = slab[zi].astype(F32)
    g[c, x, y] = stage[...].astype(BF16)

    half = (D // 2) // LANES * LANES
    cuts = (pl.ds(0, half), pl.ds(half, g.shape[-1] - half))
    gcuts = (pl.ds(0, half), pl.ds(half, D - half))
    passed = []

    def share(slot, where):
        for k in range(1, C):
            i = len(passed)
            passed.append(send(g.at[(c,) + where], g.at[(c,) + where], cs.at[i], cr.at[i],
                               device(z, y, x, lax.rem(c + k, C))))

    def plane_device(part, k1, k2):
        if part == 0:
            return device(z, lax.rem(y + k1, Y), lax.rem(x + k2, X), c)
        return device(z, lax.rem(y + k2, Y), lax.rem(x + k1, X), c)

    sizes = ((Y, X), (X, Y))
    mine = ((y, x), (x, y))

    def block(part, a, b):
        return (b, a) if part == 0 else (a, b)

    first, second = [[], []], [[], []]
    for part in (0, 1):
        a, b = mine[part]
        where = block(part, a, b) + (slice(None), cuts[part])
        for k in range(1, sizes[part][0]):
            first[part].append(send(g.at[(c,) + where], g.at[(c,) + where], s1.at[part, k], r1.at[part, k],
                                    plane_device(part, k, 0)))
    for part in (0, 1):
        share(part, block(part, *mine[part]) + (slice(None), cuts[part]))
    for part in (0, 1):
        a, b = mine[part]
        for copy in first[part]:
            copy.wait_recv()
        where = block(part, slice(None), b) + (slice(None), cuts[part])
        for k in range(1, sizes[part][1]):
            second[part].append(send(g.at[(c,) + where], g.at[(c,) + where], s2.at[part, k], r2.at[part, k],
                                     plane_device(part, 0, k)))
    for part in (0, 1):
        a, b = mine[part]
        for k in range(1, sizes[part][0]):
            share(part, block(part, lax.rem(a + k, sizes[part][0]), b) + (slice(None), cuts[part]))
    for part in (0, 1):
        a, b = mine[part]
        for k in range(1, sizes[part][1]):
            second[part][k - 1].wait_recv()
            came = lax.rem(b + sizes[part][1] - k, sizes[part][1])
            share(part, block(part, slice(None), came) + (slice(None), cuts[part]))
    load.wait()
    for copy in passed:
        copy.wait_recv()

    kk = step_of(D, 512)
    logit[...] = jnp.zeros(logit.shape, F32)

    def add_depth(i, carry):
        cols = pl.ds(pl.multiple_of(i * kk, kk), kk)
        rows = g[:, :, :, :, cols].reshape(T, kk)
        logit[...] += lax.dot_general(wt[:, cols], rows, (((1,), (1,)), ((), ())), preferred_element_type=F32)
        return carry

    lax.fori_loop(0, D // kk, add_depth, 0)
    meta = g[:, :, :, :, D:D + LANES].reshape(T, LANES).astype(F32).T
    action = meta[0:1] + 256.0 * meta[1:2] + 65536.0 * meta[2:3]
    old, advant, weights = meta[3:4], meta[4:5], meta[5:6]

    logits = logit[...]
    column = (lax.broadcasted_iota(jnp.int32, (width, T), 0) + me * width).astype(F32)
    matches = column == action
    peak = jnp.max(logits, axis=0, keepdims=True)
    shifted = jnp.exp(logits - peak)
    own[0:1] = peak
    own[1:2] = jnp.sum(shifted, axis=0, keepdims=True)
    own[2:3] = jnp.sum(shifted * logits, axis=0, keepdims=True)
    own[3:4] = jnp.sum(jnp.where(matches, logits, 0.0), axis=0, keepdims=True)
    stats[0] = own[...]

    def stat_copy(k):
        return pltpu.make_async_remote_copy(
            src_ref=own, dst_ref=stats.at[k], send_sem=ss.at[k], recv_sem=sr.at[k],
            device_id=at_offset(k), device_id_type=MESH
        )

    def tell(k, carry):
        stat_copy(k).start()
        return carry

    def hear(k, carry):
        stat_copy(k).wait()
        return carry

    lax.fori_loop(1, n, tell, 0)
    lax.fori_loop(1, n, hear, 0)
    every = stats[...]
    top = jnp.max(every[:, 0:1, :], axis=0)
    total = jnp.sum(every * jnp.exp(every[:, 0:1, :] - top[None]), axis=0)
    target = jnp.sum(every[:, 3:4, :], axis=0)
    sumexp, moment = total[1:2], total[2:3]
    lse = top + jnp.log(sumexp)
    mean_logit = moment / sumexp
    ratio = jnp.exp(target - lse - old)
    clipped = ((advant > 0.0) & (ratio > 1.2)) | ((advant < 0.0) & (ratio < 0.8))
    active = jnp.where(clipped, 0.0, 1.0)
    policy = -advant * ratio * active * weights
    logits = logit[...]
    probability = jnp.exp(logits - lse)
    onehot = jnp.where(matches, 1.0, 0.0)
    dt = policy * (onehot - probability) + 0.05 * weights * probability * (logits - mean_logit)
    dt_ref[...] = dt.astype(BF16)
    d = dt.T.astype(BF16)

    halves = []
    for part in (0, 1):
        start, size = gcuts[part].start, gcuts[part].size
        cc = step_of(size, 512)

        def columns_of(i, carry):
            cols = pl.ds(pl.multiple_of(start + i * cc, LANES), cc)
            piece = jnp.dot(d, wt[:, cols], preferred_element_type=F32)
            pb[:, :, :, :, cols] = piece.astype(BF16).reshape(C, X, Y, R, cc)
            return carry

        lax.fori_loop(0, size // cc, columns_of, 0)
        halves.append([
            send(pb.at[lax.rem(c + k, C), :, :, :, gcuts[part]], rc.at[k, :, :, :, gcuts[part]],
                 ks.at[part, k], kr.at[part, k], device(z, y, x, lax.rem(c + k, C)))
            for k in range(1, C)
        ])

    lands1, lands2 = (ra1, rb1), (ra2, rb2)
    for part in (0, 1):
        cols = gcuts[part]
        for copy in halves[part]:
            copy.wait_recv()
        acc = pb[c, :, :, :, cols].astype(F32)
        for k in range(1, C):
            acc = acc + rc[k, :, :, :, cols].astype(F32)
        pb[c, :, :, :, cols] = acc.astype(BF16)
        a, b = mine[part]
        second[part] = []
        for k in range(1, sizes[part][1]):
            other = lax.rem(b + k, sizes[part][1])
            second[part].append(send(pb.at[(c,) + block(part, slice(None), other) + (slice(None), cols)],
                                     lands1[part].at[k], t1s.at[part, k], t1r.at[part, k], plane_device(part, 0, k)))
    for part in (0, 1):
        cols = gcuts[part]
        a, b = mine[part]
        here = (c,) + block(part, slice(None), b) + (slice(None), cols)
        for copy in second[part]:
            copy.wait_recv()
        acc = pb[here].astype(F32)
        for k in range(1, sizes[part][1]):
            acc = acc + lands1[part][k].astype(F32)
        pb[here] = acc.astype(BF16)
        first[part] = []
        for k in range(1, sizes[part][0]):
            other = lax.rem(a + k, sizes[part][0])
            first[part].append(send(pb.at[(c,) + block(part, other, b) + (slice(None), cols)],
                                    lands2[part].at[k], t2s.at[part, k], t2r.at[part, k], plane_device(part, k, 0)))
    for part in (0, 1):
        cols = gcuts[part]
        for copy in first[part]:
            copy.wait_recv()
        acc = pb[c, x, y, :, cols].astype(F32)
        for k in range(1, sizes[part][0]):
            acc = acc + lands2[part][k].astype(F32)
        stage[:, cols] = acc
    for zi in range(Z):
        q[zi] = stage[zi * rp:(zi + 1) * rp, 0:D].astype(BF16)
    line = [
        send(q.at[lax.rem(z + k, Z)], rz.at[k], us.at[k], ur.at[k], device(lax.rem(z + k, Z), y, x, c))
        for k in range(1, Z)
    ]
    gall_ref[...] = g[:, :, :, :, 0:D].reshape(T, D)
    acc = q[z].astype(F32)
    for k in range(1, Z):
        line[k - 1].wait_recv()
        acc = acc + rz[k].astype(F32)
    gh_ref[...] = acc[0:real]
    for copy in started:
        copy.wait_send()


def per_device(dims, hidden, head_weight, actions, old_logp, advantage, loss_mask):
    Z, Y, X, C = dims
    n = Z * Y * X * C
    real, D = hidden.shape
    width = head_weight.shape[1]
    rp = -(-real // 4) * 4
    while Z * rp % 16:
        rp += 4
    R, T = Z * rp, n * rp
    digits = (actions % 256, actions // 256 % 256, actions // 65536)
    vectors = [v.astype(BF16) for v in digits] + [old_logp, advantage, loss_mask.astype(BF16)]
    meta = jnp.pad(jnp.stack(vectors, axis=1), ((0, 0), (0, LANES - len(vectors))))
    hx = jnp.pad(jnp.concatenate([hidden, meta], axis=1), ((0, rp - real), (0, 0)))
    half = (D // 2) // LANES * LANES
    vmem = pl.BlockSpec(memory_space=pltpu.VMEM)
    dma = pltpu.SemaphoreType.DMA
    most = max(X, Y, Z, C)
    shared = (C - 1) * (2 + (Y - 1) + (X - 1) + (X - 1) + (Y - 1))
    grad_hidden, dt, gall = pl.pallas_call(
        functools.partial(kernel, dims, real),
        out_shape=(
            jax.ShapeDtypeStruct((real, D), F32),
            jax.ShapeDtypeStruct((width, T), BF16),
            jax.ShapeDtypeStruct((T, D), BF16),
        ),
        in_specs=[vmem, pl.BlockSpec(memory_space=pl.ANY)],
        out_specs=(vmem, vmem, vmem),
        scratch_shapes=[
            pltpu.VMEM((width, D), BF16),
            pltpu.VMEM((Z, rp, D + LANES), BF16),
            pltpu.VMEM((R, D + LANES), F32),
            pltpu.VMEM((C, X, Y, R, D + LANES), BF16),
            pltpu.VMEM((4, T), F32),
            pltpu.VMEM((n, 4, T), F32),
            pltpu.VMEM((width, T), F32),
            pltpu.VMEM((C, X, Y, R, D), BF16),
            pltpu.VMEM((C, X, Y, R, D), BF16),
            pltpu.VMEM((X, Y, R, half), BF16),
            pltpu.VMEM((Y, R, half), BF16),
            pltpu.VMEM((Y, X, R, D - half), BF16),
            pltpu.VMEM((X, R, D - half), BF16),
            pltpu.VMEM((Z, rp, D), BF16),
            pltpu.VMEM((Z, rp, D), BF16),
            dma,
            dma((Z,)), dma((Z,)),
            dma((2, most)), dma((2, most)),
            dma((2, most)), dma((2, most)),
            dma((max(shared, 1),)), dma((max(shared, 1),)),
            dma((n,)), dma((n,)),
            dma((2, most)), dma((2, most)),
            dma((2, most)), dma((2, most)),
            dma((2, most)), dma((2, most)),
            dma((Z,)), dma((Z,)),
        ],
        compiler_params=pltpu.CompilerParams(
            collective_id=0, has_side_effects=True, vmem_limit_bytes=60 * 1024 * 1024
        ),
    )(hx, head_weight.T)
    grad_weight = lax.dot_general(
        gall, dt, (((0,), (1,)), ((), ())), preferred_element_type=F32
    ).astype(BF16)
    return (grad_weight, grad_hidden)


def solution(mesh):
    tok, voc = mesh.shape["tok"], mesh.shape["voc"]
    inner = 2 if tok % 2 == 0 else 1
    cores = 2 if voc % 2 == 0 else 1
    dims = (tok // inner, inner, voc // cores, cores)
    placed = (
        P(("tok", "voc"), None),
        P(None, ("tok", "voc")),
        P(("tok", "voc")),
        P(("tok", "voc")),
        P(("tok", "voc")),
        P(("tok", "voc")),
    )
    return jax.shard_map(
        functools.partial(per_device, dims),
        mesh=mesh,
        in_specs=placed,
        out_specs=(P(None, ("tok", "voc")), P(("tok", "voc"), None)),
        check_vma=False,
    )
```

```python
import functools
import math

import jax
import jax.numpy as jnp
from jax import lax
from jax.experimental import pallas as pl
from jax.experimental.pallas import tpu as pltpu
from jax.sharding import PartitionSpec as P

MESH = pl.DeviceIdType.MESH
F32, BF16 = jnp.float32, jnp.bfloat16
LANES = 128


def step_of(size, most):
    best = LANES
    for k in range(LANES, most + 1, LANES):
        if size % k == 0:
            best = k
    return best


def kernel(dims, real, hidden_ref, action_ref, mask_ref, pair_ref, wt_hbm, gh_ref, dt_ref, gall_ref,
           wt, hx_ref, slab, stage, g, own, stats, logit, pb, rc, sb, ra1, ra2, rb1, rb2, q, qf, rz,
           w_sem, zs, zr, s1, r1, s2, r2, cs, cr, ss, sr, ks, kr, t1s, t1r, t2s, t2r, us, ur):
    Z, Y, X, C = dims
    n = Z * Y * X * C
    V = X * C
    rp = hx_ref.shape[0]
    width, D = wt.shape
    R = Z * rp
    T = n * rp
    tok, voc = lax.axis_index("tok"), lax.axis_index("voc")
    z, y = tok // Y, lax.rem(tok, Y)
    x, c = voc // C, lax.rem(voc, C)
    me = tok * V + voc

    load = pltpu.make_async_copy(wt_hbm, wt, w_sem)
    load.start()

    def device(zz, yy, xx, cc):
        return (zz * Y + yy, xx * C + cc)

    def at_offset(k):
        other = lax.rem(me + k, n)
        return (other // V, lax.rem(other, V))

    barrier = pltpu.get_barrier_semaphore()

    def greet(k, carry):
        pl.semaphore_signal(barrier, inc=1, device_id=at_offset(k), device_id_type=MESH)
        return carry

    lax.fori_loop(1, n, greet, 0)

    lane = lax.broadcasted_iota(jnp.int32, (1, LANES), 1)
    stage[0:rp, :] = jnp.zeros((rp, stage.shape[1]), F32)
    stage[0:real, 0:D] = hidden_ref[...].astype(F32)
    for r in range(real):
        a = action_ref[r]
        low, rest = lax.rem(a, 256), a // 256
        whole = jnp.zeros((1, LANES), jnp.int32)
        for at, value in enumerate((low, lax.rem(rest, 256), rest // 256)):
            whole = jnp.where(lane == at, value, whole)
        whole = jnp.where(lane == 5, mask_ref[r], whole)
        extra = whole.astype(F32)
        extra = jnp.where(lane == 3, pair_ref[r], extra)
        stage[r:r + 1, D:D + LANES] = jnp.where(lane == 4, pair_ref[real + r], extra)
    hx_ref[...] = stage[0:rp, :].astype(BF16)
    pl.semaphore_wait(barrier, n - 1)

    started = []

    def send(src, dst, ssem, rsem, dev):
        copy = pltpu.make_async_remote_copy(
            src_ref=src, dst_ref=dst, send_sem=ssem, recv_sem=rsem, device_id=dev, device_id_type=MESH
        )
        copy.start()
        started.append(copy)
        return copy

    line = [
        send(hx_ref, slab.at[z], zs.at[k], zr.at[k], device(lax.rem(z + k, Z), y, x, c))
        for k in range(1, Z)
    ]
    slab[z] = hx_ref[...]
    for copy in line:
        copy.wait_recv()
    for zi in range(Z):
        stage[zi * rp:(zi + 1) * rp, :] = slab[zi].astype(F32)
    g[c, x, y] = stage[...].astype(BF16)

    half = (D // 2) // LANES * LANES
    cuts = (pl.ds(0, half), pl.ds(half, g.shape[-1] - half))
    gcuts = (pl.ds(0, half), pl.ds(half, D - half))
    passed = []

    def share(slot, where):
        for k in range(1, C):
            i = len(passed)
            passed.append(send(g.at[(c,) + where], g.at[(c,) + where], cs.at[i], cr.at[i],
                               device(z, y, x, lax.rem(c + k, C))))

    def plane_device(part, k1, k2):
        if part == 0:
            return device(z, lax.rem(y + k1, Y), lax.rem(x + k2, X), c)
        return device(z, lax.rem(y + k2, Y), lax.rem(x + k1, X), c)

    sizes = ((Y, X), (X, Y))
    mine = ((y, x), (x, y))

    def block(part, a, b):
        return (b, a) if part == 0 else (a, b)

    first, second = [[], []], [[], []]
    for part in (0, 1):
        a, b = mine[part]
        where = block(part, a, b) + (slice(None), cuts[part])
        for k in range(1, sizes[part][0]):
            first[part].append(send(g.at[(c,) + where], g.at[(c,) + where], s1.at[part, k], r1.at[part, k],
                                    plane_device(part, k, 0)))
    for part in (0, 1):
        share(part, block(part, *mine[part]) + (slice(None), cuts[part]))
    for part in (0, 1):
        a, b = mine[part]
        for copy in first[part]:
            copy.wait_recv()
        where = block(part, slice(None), b) + (slice(None), cuts[part])
        for k in range(1, sizes[part][1]):
            second[part].append(send(g.at[(c,) + where], g.at[(c,) + where], s2.at[part, k], r2.at[part, k],
                                     plane_device(part, 0, k)))
    for part in (0, 1):
        a, b = mine[part]
        for k in range(1, sizes[part][0]):
            share(part, block(part, lax.rem(a + k, sizes[part][0]), b) + (slice(None), cuts[part]))
    for part in (0, 1):
        a, b = mine[part]
        for k in range(1, sizes[part][1]):
            second[part][k - 1].wait_recv()
            came = lax.rem(b + sizes[part][1] - k, sizes[part][1])
            share(part, block(part, slice(None), came) + (slice(None), cuts[part]))
    load.wait()
    for copy in passed:
        copy.wait_recv()

    kk = step_of(D, 512)
    logit[...] = jnp.zeros(logit.shape, F32)

    def add_depth(i, carry):
        cols = pl.ds(pl.multiple_of(i * kk, kk), kk)
        rows = g[:, :, :, :, cols].reshape(T, kk)
        logit[...] += lax.dot_general(wt[:, cols], rows, (((1,), (1,)), ((), ())), preferred_element_type=F32)
        return carry

    lax.fori_loop(0, D // kk, add_depth, 0)
    meta = g[:, :, :, :, D:D + LANES].reshape(T, LANES).astype(F32).T
    action = meta[0:1] + 256.0 * meta[1:2] + 65536.0 * meta[2:3]
    old, advant, weights = meta[3:4], meta[4:5], meta[5:6]

    logits = logit[...]
    column = (lax.broadcasted_iota(jnp.int32, (width, T), 0) + me * width).astype(F32)
    matches = column == action
    peak = jnp.max(logits, axis=0, keepdims=True)
    shifted = jnp.exp(logits - peak)
    own[0:1] = peak
    own[1:2] = jnp.sum(shifted, axis=0, keepdims=True)
    own[2:3] = jnp.sum(shifted * logits, axis=0, keepdims=True)
    own[3:4] = jnp.sum(jnp.where(matches, logits, 0.0), axis=0, keepdims=True)
    stats[0] = own[...]

    def stat_copy(k):
        return pltpu.make_async_remote_copy(
            src_ref=own, dst_ref=stats.at[k], send_sem=ss.at[k], recv_sem=sr.at[k],
            device_id=at_offset(k), device_id_type=MESH
        )

    def tell(k, carry):
        stat_copy(k).start()
        return carry

    def hear(k, carry):
        stat_copy(k).wait()
        return carry

    lax.fori_loop(1, n, tell, 0)
    lax.fori_loop(1, n, hear, 0)
    every = stats[...]
    top = jnp.max(every[:, 0:1, :], axis=0)
    total = jnp.sum(every * jnp.exp(every[:, 0:1, :] - top[None]), axis=0)
    target = jnp.sum(every[:, 3:4, :], axis=0)
    sumexp, moment = total[1:2], total[2:3]
    lse = top + jnp.log(sumexp)
    mean_logit = moment / sumexp
    ratio = jnp.exp(target - lse - old)
    clipped = ((advant > 0.0) & (ratio > 1.2)) | ((advant < 0.0) & (ratio < 0.8))
    active = jnp.where(clipped, 0.0, 1.0)
    policy = -advant * ratio * active * weights
    logits = logit[...]
    probability = jnp.exp(logits - lse)
    onehot = jnp.where(matches, 1.0, 0.0)
    dt = policy * (onehot - probability) + 0.05 * weights * probability * (logits - mean_logit)
    dt_ref[...] = dt.astype(BF16)
    d = dt.T.astype(BF16)

    halves = []
    for part in (0, 1):
        start, size = gcuts[part].start, gcuts[part].size
        cc = step_of(size, 512)

        def columns_of(i, carry):
            cols = pl.ds(pl.multiple_of(start + i * cc, LANES), cc)
            piece = jnp.dot(d, wt[:, cols], preferred_element_type=F32)
            pb[:, :, :, :, cols] = piece.reshape(C, X, Y, R, cc)
            return carry

        lax.fori_loop(0, size // cc, columns_of, 0)
        halves.append([
            send(pb.at[lax.rem(c + k, C), :, :, :, gcuts[part]], rc.at[k - 1, :, :, :, gcuts[part]],
                 ks.at[part, k], kr.at[part, k], device(z, y, x, lax.rem(c + k, C)))
            for k in range(1, C)
        ])

    lands1, lands2 = (ra1, rb1), (ra2, rb2)
    for part in (0, 1):
        cols = gcuts[part]
        for copy in halves[part]:
            copy.wait_recv()
        acc = pb[c, :, :, :, cols]
        for k in range(1, C):
            acc = acc + rc[k - 1, :, :, :, cols]
        pb[c, :, :, :, cols] = acc
        sb[:, :, :, cols] = acc.astype(BF16)
        a, b = mine[part]
        second[part] = []
        for k in range(1, sizes[part][1]):
            other = lax.rem(b + k, sizes[part][1])
            second[part].append(send(sb.at[block(part, slice(None), other) + (slice(None), cols)],
                                     lands1[part].at[k - 1], t1s.at[part, k], t1r.at[part, k], plane_device(part, 0, k)))
    for part in (0, 1):
        cols = gcuts[part]
        a, b = mine[part]
        here = block(part, slice(None), b) + (slice(None), cols)
        for copy in second[part]:
            copy.wait_recv()
        acc = pb[(c,) + here]
        for k in range(1, sizes[part][1]):
            acc = acc + lands1[part][k - 1].astype(F32)
        pb[(c,) + here] = acc
        sb[here] = acc.astype(BF16)
        first[part] = []
        for k in range(1, sizes[part][0]):
            other = lax.rem(a + k, sizes[part][0])
            first[part].append(send(sb.at[block(part, other, b) + (slice(None), cols)],
                                    lands2[part].at[k - 1], t2s.at[part, k], t2r.at[part, k], plane_device(part, k, 0)))
    for part in (0, 1):
        cols = gcuts[part]
        for copy in first[part]:
            copy.wait_recv()
        acc = pb[c, x, y, :, cols]
        for k in range(1, sizes[part][0]):
            acc = acc + lands2[part][k - 1].astype(F32)
        stage[:, cols] = acc
    for zi in range(Z):
        qf[zi] = stage[zi * rp:(zi + 1) * rp, 0:D]
        q[zi] = stage[zi * rp:(zi + 1) * rp, 0:D].astype(BF16)
    line = [
        send(q.at[lax.rem(z + k, Z)], rz.at[k], us.at[k], ur.at[k], device(lax.rem(z + k, Z), y, x, c))
        for k in range(1, Z)
    ]
    gall_ref[...] = g[:, :, :, :, 0:D].reshape(T, D)
    acc = qf[z]
    for k in range(1, Z):
        line[k - 1].wait_recv()
        acc = acc + rz[k].astype(F32)
    gh_ref[...] = acc[0:real]
    for copy in started:
        copy.wait_send()


def per_device(dims, hidden, head_weight, actions, old_logp, advantage, loss_mask):
    Z, Y, X, C = dims
    n = Z * Y * X * C
    real, D = hidden.shape
    width = head_weight.shape[1]
    rp = real
    while Z * rp % 16:
        rp += 1
    R, T = Z * rp, n * rp
    pair = jnp.concatenate([old_logp, advantage]).astype(F32)
    half = (D // 2) // LANES * LANES
    vmem = pl.BlockSpec(memory_space=pltpu.VMEM)
    smem = pl.BlockSpec(memory_space=pltpu.SMEM)
    dma = pltpu.SemaphoreType.DMA
    most = max(X, Y, Z, C)
    shared = (C - 1) * (2 + (Y - 1) + (X - 1) + (X - 1) + (Y - 1))
    buffers = [
        pltpu.VMEM((width, D), BF16),
        pltpu.VMEM((rp, D + LANES), BF16),
        pltpu.VMEM((Z, rp, D + LANES), BF16),
        pltpu.VMEM((R, D + LANES), F32),
        pltpu.VMEM((C, X, Y, R, D + LANES), BF16),
        pltpu.VMEM((4, T), F32),
        pltpu.VMEM((n, 4, T), F32),
        pltpu.VMEM((width, T), F32),
        pltpu.VMEM((C, X, Y, R, D), F32),
        pltpu.VMEM((max(C - 1, 1), X, Y, R, D), F32),
        pltpu.VMEM((X, Y, R, D), BF16),
        pltpu.VMEM((max(X - 1, 1), Y, R, half), BF16),
        pltpu.VMEM((max(Y - 1, 1), R, half), BF16),
        pltpu.VMEM((max(Y - 1, 1), X, R, D - half), BF16),
        pltpu.VMEM((max(X - 1, 1), R, D - half), BF16),
        pltpu.VMEM((Z, rp, D), BF16),
        pltpu.VMEM((Z, rp, D), F32),
        pltpu.VMEM((Z, rp, D), BF16),
    ]
    taken = sum(math.prod(b.shape) * b.dtype.itemsize for b in buffers) + 2 * (width + D) * T
    grant = min(taken * 5 // 4 + (8 << 20), 60 * 1024 * 1024)
    grad_hidden, dt, gall = pl.pallas_call(
        functools.partial(kernel, dims, real),
        out_shape=(
            jax.ShapeDtypeStruct((real, D), F32),
            jax.ShapeDtypeStruct((width, T), BF16),
            jax.ShapeDtypeStruct((T, D), BF16),
        ),
        in_specs=[vmem, smem, smem, smem, pl.BlockSpec(memory_space=pltpu.HBM)],
        out_specs=(vmem, vmem, vmem),
        scratch_shapes=[
            *buffers,
            dma,
            dma((Z,)), dma((Z,)),
            dma((2, most)), dma((2, most)),
            dma((2, most)), dma((2, most)),
            dma((max(shared, 1),)), dma((max(shared, 1),)),
            dma((n,)), dma((n,)),
            dma((2, most)), dma((2, most)),
            dma((2, most)), dma((2, most)),
            dma((2, most)), dma((2, most)),
            dma((Z,)), dma((Z,)),
        ],
        compiler_params=pltpu.CompilerParams(
            collective_id=0, has_side_effects=True, vmem_limit_bytes=grant
        ),
    )(hidden, actions, loss_mask, pair, head_weight.T)
    grad_weight = lax.dot_general(
        gall, dt, (((0,), (1,)), ((), ())), preferred_element_type=F32
    ).astype(BF16)
    return (grad_weight, grad_hidden)


def solution(mesh):
    tok, voc = mesh.shape["tok"], mesh.shape["voc"]
    inner = 2 if tok % 2 == 0 else 1
    cores = 2 if voc % 2 == 0 else 1
    dims = (tok // inner, inner, voc // cores, cores)
    placed = (
        P(("tok", "voc"), None),
        P(None, ("tok", "voc")),
        P(("tok", "voc")),
        P(("tok", "voc")),
        P(("tok", "voc")),
        P(("tok", "voc")),
    )
    return jax.shard_map(
        functools.partial(per_device, dims),
        mesh=mesh,
        in_specs=placed,
        out_specs=(P(None, ("tok", "voc")), P(("tok", "voc"), None)),
        check_vma=False,
    )
```

```python
import functools
import math

import jax
import jax.numpy as jnp
from jax import lax
from jax.experimental import pallas as pl
from jax.experimental.pallas import tpu as pltpu
from jax.sharding import PartitionSpec as P

MESH = pl.DeviceIdType.MESH
F32, BF16 = jnp.float32, jnp.bfloat16
LANES = 128
PARTS = 4


def step_of(size, most):
    best = LANES
    for k in range(LANES, most + 1, LANES):
        if size % k == 0:
            best = k
    return best


def waves(parts, stages, lag):
    pairs = [(p, s) for p in range(parts) for s in range(stages)]
    return sorted(pairs, key=lambda ps: (ps[0] + lag * ps[1], -ps[1]))


def part_columns(D, parts):
    size = D // parts // LANES * LANES
    edges = [p * size for p in range(parts)] + [D]
    return list(zip(edges[:-1], edges[1:]))


def kernel(dims, real, parts, hidden_hbm, action_hbm, mask_hbm, old_hbm, advant_hbm, wt_hbm, gh_ref, dt_ref, gall_ref,
           hidden_ref, action_ref, mask_ref, old_ref, advant_ref,
           wt, hx_ref, slab, stage, g, own, stats, logit, pb, rc, sb, q, qf, rz,
           in_sem, w_sem, zs, zr, s1, r1, s2, r2, cs, cr, ss, sr, ks, kr, t1s, t1r, t2s, t2r, us, ur, *lands):
    Z, Y, X, C = dims
    n = Z * Y * X * C
    V = X * C
    rp = hx_ref.shape[0]
    width, D = wt.shape
    R = Z * rp
    T = n * rp
    tok, voc = lax.axis_index("tok"), lax.axis_index("voc")
    z, y = tok // Y, lax.rem(tok, Y)
    x, c = voc // C, lax.rem(voc, C)
    me = tok * V + voc

    inputs = [
        pltpu.make_async_copy(src, dst, in_sem.at[i])
        for i, (src, dst) in enumerate((
            (hidden_hbm, hidden_ref), (action_hbm, action_ref), (mask_hbm, mask_ref),
            (old_hbm, old_ref), (advant_hbm, advant_ref),
        ))
    ]
    for copy in inputs:
        copy.start()
    load = pltpu.make_async_copy(wt_hbm, wt, w_sem)
    load.start()

    def device(zz, yy, xx, cc):
        return (zz * Y + yy, xx * C + cc)

    def at_offset(k):
        other = lax.rem(me + k, n)
        return (other // V, lax.rem(other, V))

    barrier = pltpu.get_barrier_semaphore()

    def greet(k, carry):
        pl.semaphore_signal(barrier, inc=1, device_id=at_offset(k), device_id_type=MESH)
        return carry

    lax.fori_loop(1, n, greet, 0)

    for copy in inputs:
        copy.wait()
    lane = lax.broadcasted_iota(jnp.int32, (1, LANES), 1)
    stage[0:rp, :] = jnp.zeros((rp, stage.shape[1]), F32)
    stage[0:real, 0:D] = hidden_ref[...].astype(F32)
    spot = lax.broadcasted_iota(jnp.int32, (1, real), 1)
    olds = old_ref[...].reshape(1, real).astype(F32)
    advants = advant_ref[...].reshape(1, real).astype(F32)
    for r in range(real):
        a = action_ref[r]
        low, rest = lax.rem(a, 256), a // 256
        whole = jnp.zeros((1, LANES), jnp.int32)
        for at, value in enumerate((low, lax.rem(rest, 256), rest // 256)):
            whole = jnp.where(lane == at, value, whole)
        whole = jnp.where(lane == 5, mask_ref[r], whole)
        extra = whole.astype(F32)
        for at, values in ((3, olds), (4, advants)):
            value = jnp.sum(jnp.where(spot == r, values, 0.0), axis=1, keepdims=True)
            extra = jnp.where(lane == at, value, extra)
        stage[r:r + 1, D:D + LANES] = extra
    hx_ref[...] = stage[0:rp, :].astype(BF16)
    pl.semaphore_wait(barrier, n - 1)

    started = []

    def send(src, dst, ssem, rsem, dev):
        copy = pltpu.make_async_remote_copy(
            src_ref=src, dst_ref=dst, send_sem=ssem, recv_sem=rsem, device_id=dev, device_id_type=MESH
        )
        copy.start()
        started.append(copy)
        return copy

    spans = part_columns(D, parts)
    gcuts = [pl.ds(a, b - a) for a, b in spans]
    cuts = gcuts[:-1] + [pl.ds(spans[-1][0], D + LANES - spans[-1][0])]
    sizes = [(Y, X) if p % 2 == 0 else (X, Y) for p in range(parts)]
    mine = [(y, x) if p % 2 == 0 else (x, y) for p in range(parts)]

    def block(p, a, b):
        return (b, a) if p % 2 == 0 else (a, b)

    def plane_device(p, k1, k2):
        dx, dy = block(p, k1, k2)
        return device(z, lax.rem(y + dy, Y), lax.rem(x + dx, X), c)

    passed = [[] for _ in range(parts)]

    def share(p, where):
        for k in range(1, C):
            i = len(passed[p])
            passed[p].append(send(g.at[(c,) + where], g.at[(c,) + where], cs.at[p, i], cr.at[p, i],
                                  device(z, y, x, lax.rem(c + k, C))))

    line = [
        [send(hx_ref.at[:, cuts[p]], slab.at[z, :, cuts[p]], zs.at[p, k], zr.at[p, k],
              device(lax.rem(z + k, Z), y, x, c)) for k in range(1, Z)]
        for p in range(parts)
    ]
    slab[z] = hx_ref[...]
    first, second = [[] for _ in range(parts)], [[] for _ in range(parts)]

    def multiply(p):
        begin, end = spans[p]
        kk = step_of(end - begin, 512)
        for at in range(begin, end, kk):
            cols = pl.ds(at, kk)
            rows = g[:, :, :, :, cols].reshape(T, kk)
            term = lax.dot_general(wt[:, cols], rows, (((1,), (1,)), ((), ())), preferred_element_type=F32)
            logit[...] = term if at == 0 else logit[...] + term

    for p, s in waves(parts, 4, 3):
        a, b = mine[p]
        if s == 0:
            for copy in line[p]:
                copy.wait_recv()
            for zi in range(Z):
                stage[zi * rp:(zi + 1) * rp, cuts[p]] = slab[zi, :, cuts[p]].astype(F32)
            g[c, x, y, :, cuts[p]] = stage[:, cuts[p]].astype(BF16)
            where = block(p, a, b) + (slice(None), cuts[p])
            for k in range(1, sizes[p][0]):
                first[p].append(send(g.at[(c,) + where], g.at[(c,) + where], s1.at[p, k], r1.at[p, k],
                                     plane_device(p, k, 0)))
            share(p, where)
        elif s == 1:
            for copy in first[p]:
                copy.wait_recv()
            where = block(p, slice(None), b) + (slice(None), cuts[p])
            for k in range(1, sizes[p][1]):
                second[p].append(send(g.at[(c,) + where], g.at[(c,) + where], s2.at[p, k], r2.at[p, k],
                                      plane_device(p, 0, k)))
            for k in range(1, sizes[p][0]):
                share(p, block(p, lax.rem(a + k, sizes[p][0]), b) + (slice(None), cuts[p]))
        elif s == 2:
            for k in range(1, sizes[p][1]):
                second[p][k - 1].wait_recv()
                came = lax.rem(b + sizes[p][1] - k, sizes[p][1])
                share(p, block(p, slice(None), came) + (slice(None), cuts[p]))
        else:
            if p == 0:
                load.wait()
            for copy in passed[p]:
                copy.wait_recv()
            multiply(p)

    meta = g[:, :, :, :, D:D + LANES].reshape(T, LANES).astype(F32).T
    action = meta[0:1] + 256.0 * meta[1:2] + 65536.0 * meta[2:3]
    old, advant, weights = meta[3:4], meta[4:5], meta[5:6]

    logits = logit[...]
    column = (lax.broadcasted_iota(jnp.int32, (width, T), 0) + me * width).astype(F32)
    matches = column == action
    peak = jnp.max(logits, axis=0, keepdims=True)
    shifted = jnp.exp(logits - peak)
    own[0:1] = peak
    own[1:2] = jnp.sum(shifted, axis=0, keepdims=True)
    own[2:3] = jnp.sum(shifted * logits, axis=0, keepdims=True)
    own[3:4] = jnp.sum(jnp.where(matches, logits, 0.0), axis=0, keepdims=True)
    stats[0] = own[...]

    def stat_copy(k):
        return pltpu.make_async_remote_copy(
            src_ref=own, dst_ref=stats.at[k], send_sem=ss.at[k], recv_sem=sr.at[k],
            device_id=at_offset(k), device_id_type=MESH
        )

    def tell(k, carry):
        stat_copy(k).start()
        return carry

    def hear(k, carry):
        stat_copy(k).wait()
        return carry

    lax.fori_loop(1, n, tell, 0)
    lax.fori_loop(1, n, hear, 0)
    every = stats[...]
    top = jnp.max(every[:, 0:1, :], axis=0)
    total = jnp.sum(every * jnp.exp(every[:, 0:1, :] - top[None]), axis=0)
    target = jnp.sum(every[:, 3:4, :], axis=0)
    sumexp, moment = total[1:2], total[2:3]
    lse = top + jnp.log(sumexp)
    mean_logit = moment / sumexp
    ratio = jnp.exp(target - lse - old)
    clipped = ((advant > 0.0) & (ratio > 1.2)) | ((advant < 0.0) & (ratio < 0.8))
    active = jnp.where(clipped, 0.0, 1.0)
    policy = -advant * ratio * active * weights
    logits = logit[...]
    probability = jnp.exp(logits - lse)
    onehot = jnp.where(matches, 1.0, 0.0)
    dt = policy * (onehot - probability) + 0.05 * weights * probability * (logits - mean_logit)
    dt_ref[...] = dt.astype(BF16)
    d = dt.T.astype(BF16)

    halves, line = [[] for _ in range(parts)], [[] for _ in range(parts)]
    first, second = [[] for _ in range(parts)], [[] for _ in range(parts)]
    for p, s in waves(parts, 5, 3):
        a, b = mine[p]
        cols = gcuts[p]
        here = block(p, slice(None), b) + (slice(None), cols)
        if s == 0:
            begin, end = spans[p]
            cc = step_of(end - begin, 512)
            for at in range(begin, end, cc):
                piece = jnp.dot(d, wt[:, at:at + cc], preferred_element_type=F32)
                pb[:, :, :, :, at:at + cc] = piece.reshape(C, X, Y, R, cc)
            halves[p] = [
                send(pb.at[lax.rem(c + k, C), :, :, :, cols], rc.at[k - 1, :, :, :, cols],
                     ks.at[p, k], kr.at[p, k], device(z, y, x, lax.rem(c + k, C)))
                for k in range(1, C)
            ]
        elif s == 1:
            for copy in halves[p]:
                copy.wait_recv()
            acc = pb[c, :, :, :, cols]
            for k in range(1, C):
                acc = acc + rc[k - 1, :, :, :, cols]
            pb[c, :, :, :, cols] = acc
            sb[:, :, :, cols] = acc.astype(BF16)
            for k in range(1, sizes[p][1]):
                other = lax.rem(b + k, sizes[p][1])
                second[p].append(send(sb.at[block(p, slice(None), other) + (slice(None), cols)],
                                      lands[2 * p].at[k - 1], t1s.at[p, k], t1r.at[p, k], plane_device(p, 0, k)))
        elif s == 2:
            for copy in second[p]:
                copy.wait_recv()
            acc = pb[(c,) + here]
            for k in range(1, sizes[p][1]):
                acc = acc + lands[2 * p][k - 1].astype(F32)
            pb[(c,) + here] = acc
            sb[here] = acc.astype(BF16)
            for k in range(1, sizes[p][0]):
                other = lax.rem(a + k, sizes[p][0])
                first[p].append(send(sb.at[block(p, other, b) + (slice(None), cols)],
                                     lands[2 * p + 1].at[k - 1], t2s.at[p, k], t2r.at[p, k], plane_device(p, k, 0)))
            if p == 0:
                gall_ref[...] = g[:, :, :, :, 0:D].reshape(T, D)
        elif s == 3:
            for copy in first[p]:
                copy.wait_recv()
            acc = pb[c, x, y, :, cols]
            for k in range(1, sizes[p][0]):
                acc = acc + lands[2 * p + 1][k - 1].astype(F32)
            stage[:, cols] = acc
            for zi in range(Z):
                piece = stage[zi * rp:(zi + 1) * rp, cols]
                qf[zi, :, cols] = piece
                q[zi, :, cols] = piece.astype(BF16)
            line[p] = [
                send(q.at[lax.rem(z + k, Z), :, cols], rz.at[k, :, cols], us.at[p, k], ur.at[p, k],
                     device(lax.rem(z + k, Z), y, x, c))
                for k in range(1, Z)
            ]
        else:
            acc = qf[z, :, cols]
            for k in range(1, Z):
                line[p][k - 1].wait_recv()
                acc = acc + rz[k, :, cols].astype(F32)
            gh_ref[:, cols] = acc[0:real]
    for copy in started:
        copy.wait_send()


def per_device(dims, hidden, head_weight, actions, old_logp, advantage, loss_mask):
    Z, Y, X, C = dims
    n = Z * Y * X * C
    real, D = hidden.shape
    width = head_weight.shape[1]
    rp = real
    while Z * rp % 16:
        rp += 1
    R, T = Z * rp, n * rp
    parts = PARTS
    spans = part_columns(D, parts)
    vmem = pl.BlockSpec(memory_space=pltpu.VMEM)
    hbm = pl.BlockSpec(memory_space=pltpu.HBM)
    dma = pltpu.SemaphoreType.DMA
    most = max(X, Y, Z, C)
    shared = max((C - 1) * (X + Y - 1), 1)
    lands = []
    for p, (begin, end) in enumerate(spans):
        one, two = (Y, X) if p % 2 == 0 else (X, Y)
        lands.append(pltpu.VMEM((max(two - 1, 1), one, R, end - begin), BF16))
        lands.append(pltpu.VMEM((max(one - 1, 1), R, end - begin), BF16))
    buffers = [
        pltpu.VMEM((width, D), BF16),
        pltpu.VMEM((rp, D + LANES), BF16),
        pltpu.VMEM((Z, rp, D + LANES), BF16),
        pltpu.VMEM((R, D + LANES), F32),
        pltpu.VMEM((C, X, Y, R, D + LANES), BF16),
        pltpu.VMEM((4, T), F32),
        pltpu.VMEM((n, 4, T), F32),
        pltpu.VMEM((width, T), F32),
        pltpu.VMEM((C, X, Y, R, D), F32),
        pltpu.VMEM((max(C - 1, 1), X, Y, R, D), F32),
        pltpu.VMEM((X, Y, R, D), BF16),
        pltpu.VMEM((Z, rp, D), BF16),
        pltpu.VMEM((Z, rp, D), F32),
        pltpu.VMEM((Z, rp, D), BF16),
    ]
    taken = sum(math.prod(b.shape) * b.dtype.itemsize for b in buffers + lands) + 2 * (width + D) * T
    grant = min(taken * 5 // 4 + (8 << 20), 60 * 1024 * 1024)
    grad_hidden, dt, gall = pl.pallas_call(
        functools.partial(kernel, dims, real, parts),
        out_shape=(
            jax.ShapeDtypeStruct((real, D), F32),
            jax.ShapeDtypeStruct((width, T), BF16),
            jax.ShapeDtypeStruct((T, D), BF16),
        ),
        in_specs=[hbm] * 6,
        out_specs=(vmem, vmem, vmem),
        scratch_shapes=[
            pltpu.VMEM(hidden.shape, BF16),
            pltpu.SMEM(actions.shape, jnp.int32),
            pltpu.SMEM(loss_mask.shape, jnp.int32),
            pltpu.VMEM(old_logp.shape, BF16),
            pltpu.VMEM(advantage.shape, BF16),
            *buffers,
            dma((5,)),
            dma,
            dma((parts, Z)), dma((parts, Z)),
            dma((parts, most)), dma((parts, most)),
            dma((parts, most)), dma((parts, most)),
            dma((parts, shared)), dma((parts, shared)),
            dma((n,)), dma((n,)),
            dma((parts, most)), dma((parts, most)),
            dma((parts, most)), dma((parts, most)),
            dma((parts, most)), dma((parts, most)),
            dma((parts, Z)), dma((parts, Z)),
            *lands,
        ],
        compiler_params=pltpu.CompilerParams(
            collective_id=0, has_side_effects=True, vmem_limit_bytes=grant
        ),
    )(*(pltpu.with_memory_space_constraint(v, pltpu.HBM)
        for v in (hidden, actions, loss_mask, old_logp, advantage, head_weight.T)))
    grad_weight = lax.dot_general(
        gall, dt, (((0,), (1,)), ((), ())), preferred_element_type=F32
    ).astype(BF16)
    return (grad_weight, grad_hidden)


def solution(mesh):
    tok, voc = mesh.shape["tok"], mesh.shape["voc"]
    inner = 2 if tok % 2 == 0 else 1
    cores = 2 if voc % 2 == 0 else 1
    dims = (tok // inner, inner, voc // cores, cores)
    placed = (
        P(("tok", "voc"), None),
        P(None, ("tok", "voc")),
        P(("tok", "voc")),
        P(("tok", "voc")),
        P(("tok", "voc")),
        P(("tok", "voc")),
    )
    return jax.shard_map(
        functools.partial(per_device, dims),
        mesh=mesh,
        in_specs=placed,
        out_specs=(P(None, ("tok", "voc")), P(("tok", "voc"), None)),
        check_vma=False,
    )
```

```python
import functools
import math

import jax
import jax.numpy as jnp
from jax import lax
from jax.experimental import pallas as pl
from jax.experimental.pallas import tpu as pltpu
from jax.sharding import PartitionSpec as P

MESH = pl.DeviceIdType.MESH
F32, BF16 = jnp.float32, jnp.bfloat16
LANES = 128
PARTS = 2
GATHER_DELAYS = (0, 3, 6, 7.5)
SCATTER_DELAYS = (0, 3, 6, 9, 12)


def step_of(size, most):
    best = LANES
    for k in range(LANES, most + 1, LANES):
        if size % k == 0:
            best = k
    return best


def waves(parts, delays):
    pairs = [(p, s) for p in range(parts) for s in range(len(delays))]
    return sorted(pairs, key=lambda ps: (ps[0] + delays[ps[1]], -ps[1]))


def part_columns(D, parts):
    size = D // parts // LANES * LANES
    edges = [p * size for p in range(parts)] + [D]
    return list(zip(edges[:-1], edges[1:]))


def kernel(dims, real, parts, hidden_hbm, action_hbm, mask_hbm, old_hbm, advant_hbm, wt_hbm, gh_ref, dt_ref, gall_ref,
           hidden_ref, action_ref, mask_ref, old_ref, advant_ref,
           wt, hx_ref, slab, stage, g, own, stats, logit, pb, rc, sb, q, qf, rz,
           in_sem, w_sem, zs, zr, s1, r1, s2, r2, cs, cr, ss, sr, ks, kr, t1s, t1r, t2s, t2r, us, ur, *lands):
    Z, Y, X, C = dims
    n = Z * Y * X * C
    V = X * C
    rp = hx_ref.shape[0]
    width, D = wt.shape
    R = Z * rp
    T = n * rp
    tok, voc = lax.axis_index("tok"), lax.axis_index("voc")
    z, y = tok // Y, lax.rem(tok, Y)
    x, c = voc // C, lax.rem(voc, C)
    me = tok * V + voc

    inputs = [
        pltpu.make_async_copy(src, dst, in_sem.at[i])
        for i, (src, dst) in enumerate((
            (hidden_hbm, hidden_ref), (action_hbm, action_ref), (mask_hbm, mask_ref),
            (old_hbm, old_ref), (advant_hbm, advant_ref),
        ))
    ]
    for copy in inputs:
        copy.start()
    load = pltpu.make_async_copy(wt_hbm, wt, w_sem)
    load.start()

    def device(zz, yy, xx, cc):
        return (zz * Y + yy, xx * C + cc)

    def at_offset(k):
        other = lax.rem(me + k, n)
        return (other // V, lax.rem(other, V))

    barrier = pltpu.get_barrier_semaphore()

    def greet(k, carry):
        pl.semaphore_signal(barrier, inc=1, device_id=at_offset(k), device_id_type=MESH)
        return carry

    lax.fori_loop(1, n, greet, 0)

    for copy in inputs:
        copy.wait()
    lane = lax.broadcasted_iota(jnp.int32, (1, LANES), 1)
    stage[0:rp, :] = jnp.zeros((rp, stage.shape[1]), F32)
    stage[0:real, 0:D] = hidden_ref[...].astype(F32)
    spot = lax.broadcasted_iota(jnp.int32, (1, real), 1)
    olds = old_ref[...].reshape(1, real).astype(F32)
    advants = advant_ref[...].reshape(1, real).astype(F32)
    for r in range(real):
        a = action_ref[r]
        low, rest = lax.rem(a, 256), a // 256
        whole = jnp.zeros((1, LANES), jnp.int32)
        for at, value in enumerate((low, lax.rem(rest, 256), rest // 256)):
            whole = jnp.where(lane == at, value, whole)
        whole = jnp.where(lane == 5, mask_ref[r], whole)
        extra = whole.astype(F32)
        for at, values in ((3, olds), (4, advants)):
            value = jnp.sum(jnp.where(spot == r, values, 0.0), axis=1, keepdims=True)
            extra = jnp.where(lane == at, value, extra)
        stage[r:r + 1, D:D + LANES] = extra
    hx_ref[...] = stage[0:rp, :].astype(BF16)
    pl.semaphore_wait(barrier, n - 1)

    started = []

    def send(src, dst, ssem, rsem, dev):
        copy = pltpu.make_async_remote_copy(
            src_ref=src, dst_ref=dst, send_sem=ssem, recv_sem=rsem, device_id=dev, device_id_type=MESH
        )
        copy.start()
        started.append(copy)
        return copy

    spans = part_columns(D, parts)
    gcuts = [pl.ds(a, b - a) for a, b in spans]
    cuts = gcuts[:-1] + [pl.ds(spans[-1][0], D + LANES - spans[-1][0])]
    sizes = [(Y, X) if p % 2 == 0 else (X, Y) for p in range(parts)]
    mine = [(y, x) if p % 2 == 0 else (x, y) for p in range(parts)]

    def block(p, a, b):
        return (b, a) if p % 2 == 0 else (a, b)

    def plane_device(p, k1, k2):
        dx, dy = block(p, k1, k2)
        return device(z, lax.rem(y + dy, Y), lax.rem(x + dx, X), c)

    passed = [[] for _ in range(parts)]

    def share(p, where):
        for k in range(1, C):
            i = len(passed[p])
            passed[p].append(send(g.at[(c,) + where], g.at[(c,) + where], cs.at[p, i], cr.at[p, i],
                                  device(z, y, x, lax.rem(c + k, C))))

    line = [
        [send(hx_ref.at[:, cuts[p]], slab.at[z, :, cuts[p]], zs.at[p, k], zr.at[p, k],
              device(lax.rem(z + k, Z), y, x, c)) for k in range(1, Z)]
        for p in range(parts)
    ]
    slab[z] = hx_ref[...]
    first, second = [[] for _ in range(parts)], [[] for _ in range(parts)]

    def multiply(p):
        begin, end = spans[p]
        kk = step_of(end - begin, 512)
        for at in range(begin, end, kk):
            cols = pl.ds(at, kk)
            rows = g[:, :, :, :, cols].reshape(T, kk)
            term = lax.dot_general(wt[:, cols], rows, (((1,), (1,)), ((), ())), preferred_element_type=F32)
            logit[...] = term if at == 0 else logit[...] + term

    for p, s in waves(parts, GATHER_DELAYS):
        a, b = mine[p]
        if s == 0:
            for copy in line[p]:
                copy.wait_recv()
            for zi in range(Z):
                stage[zi * rp:(zi + 1) * rp, cuts[p]] = slab[zi, :, cuts[p]].astype(F32)
            g[c, x, y, :, cuts[p]] = stage[:, cuts[p]].astype(BF16)
            where = block(p, a, b) + (slice(None), cuts[p])
            for k in range(1, sizes[p][0]):
                first[p].append(send(g.at[(c,) + where], g.at[(c,) + where], s1.at[p, k], r1.at[p, k],
                                     plane_device(p, k, 0)))
            share(p, where)
        elif s == 1:
            for copy in first[p]:
                copy.wait_recv()
            where = block(p, slice(None), b) + (slice(None), cuts[p])
            for k in range(1, sizes[p][1]):
                second[p].append(send(g.at[(c,) + where], g.at[(c,) + where], s2.at[p, k], r2.at[p, k],
                                      plane_device(p, 0, k)))
            for k in range(1, sizes[p][0]):
                share(p, block(p, lax.rem(a + k, sizes[p][0]), b) + (slice(None), cuts[p]))
        elif s == 2:
            for k in range(1, sizes[p][1]):
                second[p][k - 1].wait_recv()
                came = lax.rem(b + sizes[p][1] - k, sizes[p][1])
                share(p, block(p, slice(None), came) + (slice(None), cuts[p]))
        else:
            if p == 0:
                load.wait()
            for copy in passed[p]:
                copy.wait_recv()
            multiply(p)

    meta = g[:, :, :, :, D:D + LANES].reshape(T, LANES).astype(F32).T
    action = meta[0:1] + 256.0 * meta[1:2] + 65536.0 * meta[2:3]
    old, advant, weights = meta[3:4], meta[4:5], meta[5:6]

    logits = logit[...]
    column = (lax.broadcasted_iota(jnp.int32, (width, T), 0) + me * width).astype(F32)
    matches = column == action
    peak = jnp.max(logits, axis=0, keepdims=True)
    shifted = jnp.exp(logits - peak)
    own[0:1] = peak
    own[1:2] = jnp.sum(shifted, axis=0, keepdims=True)
    own[2:3] = jnp.sum(shifted * logits, axis=0, keepdims=True)
    own[3:4] = jnp.sum(jnp.where(matches, logits, 0.0), axis=0, keepdims=True)
    stats[0] = own[...]

    def stat_copy(k):
        return pltpu.make_async_remote_copy(
            src_ref=own, dst_ref=stats.at[k], send_sem=ss.at[k], recv_sem=sr.at[k],
            device_id=at_offset(k), device_id_type=MESH
        )

    def tell(i, carry):
        stat_copy(1 + lax.rem(i + n // 4, n - 1)).start()
        return carry

    def hear(k, carry):
        stat_copy(k).wait()
        return carry

    lax.fori_loop(1, n, tell, 0)
    lax.fori_loop(1, n, hear, 0)
    every = stats[...]
    top = jnp.max(every[:, 0:1, :], axis=0)
    total = jnp.sum(every * jnp.exp(every[:, 0:1, :] - top[None]), axis=0)
    target = jnp.sum(every[:, 3:4, :], axis=0)
    sumexp, moment = total[1:2], total[2:3]
    lse = top + jnp.log(sumexp)
    mean_logit = moment / sumexp
    ratio = jnp.exp(target - lse - old)
    clipped = ((advant > 0.0) & (ratio > 1.2)) | ((advant < 0.0) & (ratio < 0.8))
    active = jnp.where(clipped, 0.0, 1.0)
    policy = -advant * ratio * active * weights
    logits = logit[...]
    probability = jnp.exp(logits - lse)
    onehot = jnp.where(matches, 1.0, 0.0)
    dt = policy * (onehot - probability) + 0.05 * weights * probability * (logits - mean_logit)
    dt_ref[...] = dt.astype(BF16)
    d = dt.T.astype(BF16)

    halves, line = [[] for _ in range(parts)], [[] for _ in range(parts)]
    first, second = [[] for _ in range(parts)], [[] for _ in range(parts)]
    for p, s in waves(parts, SCATTER_DELAYS):
        a, b = mine[p]
        cols = gcuts[p]
        here = block(p, slice(None), b) + (slice(None), cols)
        if s == 0:
            begin, end = spans[p]
            cc = step_of(end - begin, 512)
            for at in range(begin, end, cc):
                piece = jnp.dot(d, wt[:, at:at + cc], preferred_element_type=F32)
                pb[:, :, :, :, at:at + cc] = piece.reshape(C, X, Y, R, cc)
            halves[p] = [
                send(pb.at[lax.rem(c + k, C), :, :, :, cols], rc.at[k - 1, :, :, :, cols],
                     ks.at[p, k], kr.at[p, k], device(z, y, x, lax.rem(c + k, C)))
                for k in range(1, C)
            ]
        elif s == 1:
            for copy in halves[p]:
                copy.wait_recv()
            acc = pb[c, :, :, :, cols]
            for k in range(1, C):
                acc = acc + rc[k - 1, :, :, :, cols]
            pb[c, :, :, :, cols] = acc
            sb[:, :, :, cols] = acc.astype(BF16)
            for k in range(1, sizes[p][1]):
                other = lax.rem(b + k, sizes[p][1])
                second[p].append(send(sb.at[block(p, slice(None), other) + (slice(None), cols)],
                                      lands[2 * p].at[k - 1], t1s.at[p, k], t1r.at[p, k], plane_device(p, 0, k)))
        elif s == 2:
            for copy in second[p]:
                copy.wait_recv()
            acc = pb[(c,) + here]
            for k in range(1, sizes[p][1]):
                acc = acc + lands[2 * p][k - 1].astype(F32)
            pb[(c,) + here] = acc
            sb[here] = acc.astype(BF16)
            for k in range(1, sizes[p][0]):
                other = lax.rem(a + k, sizes[p][0])
                first[p].append(send(sb.at[block(p, other, b) + (slice(None), cols)],
                                     lands[2 * p + 1].at[k - 1], t2s.at[p, k], t2r.at[p, k], plane_device(p, k, 0)))
            if p == 0:
                gall_ref[...] = g[:, :, :, :, 0:D].reshape(T, D)
        elif s == 3:
            for copy in first[p]:
                copy.wait_recv()
            acc = pb[c, x, y, :, cols]
            for k in range(1, sizes[p][0]):
                acc = acc + lands[2 * p + 1][k - 1].astype(F32)
            stage[:, cols] = acc
            for zi in range(Z):
                piece = stage[zi * rp:(zi + 1) * rp, cols]
                qf[zi, :, cols] = piece
                q[zi, :, cols] = piece.astype(BF16)
            line[p] = [
                send(q.at[lax.rem(z + k, Z), :, cols], rz.at[k, :, cols], us.at[p, k], ur.at[p, k],
                     device(lax.rem(z + k, Z), y, x, c))
                for k in range(1, Z)
            ]
        else:
            acc = qf[z, :, cols]
            for k in range(1, Z):
                line[p][k - 1].wait_recv()
                acc = acc + rz[k, :, cols].astype(F32)
            gh_ref[:, cols] = acc[0:real]
    for copy in started:
        copy.wait_send()


def per_device(dims, hidden, head_weight, actions, old_logp, advantage, loss_mask):
    Z, Y, X, C = dims
    n = Z * Y * X * C
    real, D = hidden.shape
    width = head_weight.shape[1]
    rp = real
    while Z * rp % 16:
        rp += 1
    R, T = Z * rp, n * rp
    parts = PARTS
    spans = part_columns(D, parts)
    vmem = pl.BlockSpec(memory_space=pltpu.VMEM)
    hbm = pl.BlockSpec(memory_space=pltpu.HBM)
    dma = pltpu.SemaphoreType.DMA
    most = max(X, Y, Z, C)
    shared = max((C - 1) * (X + Y - 1), 1)
    lands = []
    for p, (begin, end) in enumerate(spans):
        one, two = (Y, X) if p % 2 == 0 else (X, Y)
        lands.append(pltpu.VMEM((max(two - 1, 1), one, R, end - begin), BF16))
        lands.append(pltpu.VMEM((max(one - 1, 1), R, end - begin), BF16))
    buffers = [
        pltpu.VMEM((width, D), BF16),
        pltpu.VMEM((rp, D + LANES), BF16),
        pltpu.VMEM((Z, rp, D + LANES), BF16),
        pltpu.VMEM((R, D + LANES), F32),
        pltpu.VMEM((C, X, Y, R, D + LANES), BF16),
        pltpu.VMEM((4, T), F32),
        pltpu.VMEM((n, 4, T), F32),
        pltpu.VMEM((width, T), F32),
        pltpu.VMEM((C, X, Y, R, D), F32),
        pltpu.VMEM((max(C - 1, 1), X, Y, R, D), F32),
        pltpu.VMEM((X, Y, R, D), BF16),
        pltpu.VMEM((Z, rp, D), BF16),
        pltpu.VMEM((Z, rp, D), F32),
        pltpu.VMEM((Z, rp, D), BF16),
    ]
    taken = sum(math.prod(b.shape) * b.dtype.itemsize for b in buffers + lands) + 2 * (width + D) * T
    grant = min(taken * 5 // 4 + (8 << 20), 60 * 1024 * 1024)
    grad_hidden, dt, gall = pl.pallas_call(
        functools.partial(kernel, dims, real, parts),
        out_shape=(
            jax.ShapeDtypeStruct((real, D), F32),
            jax.ShapeDtypeStruct((width, T), BF16),
            jax.ShapeDtypeStruct((T, D), BF16),
        ),
        in_specs=[hbm] * 6,
        out_specs=(vmem, vmem, vmem),
        scratch_shapes=[
            pltpu.VMEM(hidden.shape, BF16),
            pltpu.SMEM(actions.shape, jnp.int32),
            pltpu.SMEM(loss_mask.shape, jnp.int32),
            pltpu.VMEM(old_logp.shape, BF16),
            pltpu.VMEM(advantage.shape, BF16),
            *buffers,
            dma((5,)),
            dma,
            dma((parts, Z)), dma((parts, Z)),
            dma((parts, most)), dma((parts, most)),
            dma((parts, most)), dma((parts, most)),
            dma((parts, shared)), dma((parts, shared)),
            dma((n,)), dma((n,)),
            dma((parts, most)), dma((parts, most)),
            dma((parts, most)), dma((parts, most)),
            dma((parts, most)), dma((parts, most)),
            dma((parts, Z)), dma((parts, Z)),
            *lands,
        ],
        compiler_params=pltpu.CompilerParams(
            collective_id=0, has_side_effects=True, vmem_limit_bytes=grant
        ),
    )(*(pltpu.with_memory_space_constraint(v, pltpu.HBM)
        for v in (hidden, actions, loss_mask, old_logp, advantage, head_weight.T)))
    grad_weight = lax.dot_general(
        gall, dt, (((0,), (1,)), ((), ())), preferred_element_type=F32
    ).astype(BF16)
    return (grad_weight, grad_hidden)


def solution(mesh):
    tok, voc = mesh.shape["tok"], mesh.shape["voc"]
    inner = 2 if tok % 2 == 0 else 1
    cores = 2 if voc % 2 == 0 else 1
    dims = (tok // inner, inner, voc // cores, cores)
    placed = (
        P(("tok", "voc"), None),
        P(None, ("tok", "voc")),
        P(("tok", "voc")),
        P(("tok", "voc")),
        P(("tok", "voc")),
        P(("tok", "voc")),
    )
    return jax.shard_map(
        functools.partial(per_device, dims),
        mesh=mesh,
        in_specs=placed,
        out_specs=(P(None, ("tok", "voc")), P(("tok", "voc"), None)),
        check_vma=False,
    )
```

```python
import functools
import math

import jax
import jax.numpy as jnp
from jax import lax
from jax.experimental import pallas as pl
from jax.experimental.pallas import tpu as pltpu
from jax.sharding import PartitionSpec as P

MESH = pl.DeviceIdType.MESH
F32, BF16 = jnp.float32, jnp.bfloat16
LANES = 128
PARTS = 2
GATHER_DELAYS = (0, 3, 6, 7.5)
SCATTER_DELAYS = (0, 3, 6, 9, 12)


def step_of(size, most):
    best = LANES
    for k in range(LANES, most + 1, LANES):
        if size % k == 0:
            best = k
    return best


def waves(parts, delays):
    pairs = [(p, s) for p in range(parts) for s in range(len(delays))]
    return sorted(pairs, key=lambda ps: (ps[0] + delays[ps[1]], -ps[1]))


def part_columns(D, parts):
    size = D // parts // LANES * LANES
    edges = [p * size for p in range(parts)] + [D]
    return list(zip(edges[:-1], edges[1:]))


def kernel(dims, real, parts, hidden_hbm, action_hbm, mask_hbm, old_hbm, advant_hbm, wt_hbm, gh_ref, gw_ref,
           hidden_ref, action_ref, mask_ref, old_ref, advant_ref,
           wt, dt_ref, hx_ref, slab, stage, g, own, stats, logit, pb, rc, sb, q, qf, rz,
           in_sem, w_sem, zs, zr, s1, r1, s2, r2, cs, cr, ss, sr, ks, kr, t1s, t1r, t2s, t2r, us, ur, *lands):
    Z, Y, X, C = dims
    n = Z * Y * X * C
    V = X * C
    rp = hx_ref.shape[0]
    width, D = wt.shape
    R = Z * rp
    T = n * rp
    tok, voc = lax.axis_index("tok"), lax.axis_index("voc")
    z, y = tok // Y, lax.rem(tok, Y)
    x, c = voc // C, lax.rem(voc, C)
    me = tok * V + voc

    inputs = [
        pltpu.make_async_copy(src, dst, in_sem.at[i])
        for i, (src, dst) in enumerate((
            (hidden_hbm, hidden_ref), (action_hbm, action_ref), (mask_hbm, mask_ref),
            (old_hbm, old_ref), (advant_hbm, advant_ref),
        ))
    ]
    for copy in inputs:
        copy.start()
    load = pltpu.make_async_copy(wt_hbm, wt, w_sem)
    load.start()

    def device(zz, yy, xx, cc):
        return (zz * Y + yy, xx * C + cc)

    def at_offset(k):
        other = lax.rem(me + k, n)
        return (other // V, lax.rem(other, V))

    barrier = pltpu.get_barrier_semaphore()

    def greet(k, carry):
        pl.semaphore_signal(barrier, inc=1, device_id=at_offset(k), device_id_type=MESH)
        return carry

    lax.fori_loop(1, n, greet, 0)

    for copy in inputs:
        copy.wait()
    lane = lax.broadcasted_iota(jnp.int32, (1, LANES), 1)
    stage[0:rp, :] = jnp.zeros((rp, stage.shape[1]), F32)
    stage[0:real, 0:D] = hidden_ref[...].astype(F32)
    spot = lax.broadcasted_iota(jnp.int32, (1, real), 1)
    olds = old_ref[...].reshape(1, real).astype(F32)
    advants = advant_ref[...].reshape(1, real).astype(F32)
    for r in range(real):
        a = action_ref[r]
        low, rest = lax.rem(a, 256), a // 256
        whole = jnp.zeros((1, LANES), jnp.int32)
        for at, value in enumerate((low, lax.rem(rest, 256), rest // 256)):
            whole = jnp.where(lane == at, value, whole)
        whole = jnp.where(lane == 5, mask_ref[r], whole)
        extra = whole.astype(F32)
        for at, values in ((3, olds), (4, advants)):
            value = jnp.sum(jnp.where(spot == r, values, 0.0), axis=1, keepdims=True)
            extra = jnp.where(lane == at, value, extra)
        stage[r:r + 1, D:D + LANES] = extra
    hx_ref[...] = stage[0:rp, :].astype(BF16)
    pl.semaphore_wait(barrier, n - 1)

    started = []

    def send(src, dst, ssem, rsem, dev):
        copy = pltpu.make_async_remote_copy(
            src_ref=src, dst_ref=dst, send_sem=ssem, recv_sem=rsem, device_id=dev, device_id_type=MESH
        )
        copy.start()
        started.append(copy)
        return copy

    spans = part_columns(D, parts)
    gcuts = [pl.ds(a, b - a) for a, b in spans]
    cuts = gcuts[:-1] + [pl.ds(spans[-1][0], D + LANES - spans[-1][0])]
    sizes = [(Y, X) if p % 2 == 0 else (X, Y) for p in range(parts)]
    mine = [(y, x) if p % 2 == 0 else (x, y) for p in range(parts)]

    def block(p, a, b):
        return (b, a) if p % 2 == 0 else (a, b)

    def plane_device(p, k1, k2):
        dx, dy = block(p, k1, k2)
        return device(z, lax.rem(y + dy, Y), lax.rem(x + dx, X), c)

    passed = [[] for _ in range(parts)]

    def share(p, where):
        for k in range(1, C):
            i = len(passed[p])
            passed[p].append(send(g.at[(c,) + where], g.at[(c,) + where], cs.at[p, i], cr.at[p, i],
                                  device(z, y, x, lax.rem(c + k, C))))

    line = [
        send(hx_ref, slab.at[z], zs.at[0, k], zr.at[0, k], device(lax.rem(z + k, Z), y, x, c)) for k in range(1, Z)
    ]
    slab[z] = hx_ref[...]
    first, second = [[] for _ in range(parts)], [[] for _ in range(parts)]

    def multiply(p):
        begin, end = spans[p]
        kk = step_of(end - begin, 512)
        for at in range(begin, end, kk):
            cols = pl.ds(at, kk)
            rows = g[:, :, :, :, cols].reshape(T, kk)
            term = lax.dot_general(wt[:, cols], rows, (((1,), (1,)), ((), ())), preferred_element_type=F32)
            logit[...] = term if at == 0 else logit[...] + term

    for p, s in waves(parts, GATHER_DELAYS):
        a, b = mine[p]
        if s == 0:
            for copy in line if p == 0 else ():
                copy.wait_recv()
            for zi in range(Z):
                stage[zi * rp:(zi + 1) * rp, cuts[p]] = slab[zi, :, cuts[p]].astype(F32)
            g[c, x, y, :, cuts[p]] = stage[:, cuts[p]].astype(BF16)
            where = block(p, a, b) + (slice(None), cuts[p])
            for k in range(1, sizes[p][0]):
                first[p].append(send(g.at[(c,) + where], g.at[(c,) + where], s1.at[p, k], r1.at[p, k],
                                     plane_device(p, k, 0)))
            share(p, where)
        elif s == 1:
            for copy in first[p]:
                copy.wait_recv()
            where = block(p, slice(None), b) + (slice(None), cuts[p])
            for k in range(1, sizes[p][1]):
                second[p].append(send(g.at[(c,) + where], g.at[(c,) + where], s2.at[p, k], r2.at[p, k],
                                      plane_device(p, 0, k)))
            for k in range(1, sizes[p][0]):
                share(p, block(p, lax.rem(a + k, sizes[p][0]), b) + (slice(None), cuts[p]))
        elif s == 2:
            for k in range(1, sizes[p][1]):
                second[p][k - 1].wait_recv()
                came = lax.rem(b + sizes[p][1] - k, sizes[p][1])
                share(p, block(p, slice(None), came) + (slice(None), cuts[p]))
        else:
            if p == 0:
                load.wait()
            for copy in passed[p]:
                copy.wait_recv()
            multiply(p)

    meta = g[:, :, :, :, D:D + LANES].reshape(T, LANES).astype(F32).T
    action = meta[0:1] + 256.0 * meta[1:2] + 65536.0 * meta[2:3]
    old, advant, weights = meta[3:4], meta[4:5], meta[5:6]

    logits = logit[...]
    column = (lax.broadcasted_iota(jnp.int32, (width, T), 0) + me * width).astype(F32)
    matches = column == action
    peak = jnp.max(logits, axis=0, keepdims=True)
    shifted = jnp.exp(logits - peak)
    own[0:1] = peak
    own[1:2] = jnp.sum(shifted, axis=0, keepdims=True)
    own[2:3] = jnp.sum(shifted * logits, axis=0, keepdims=True)
    own[3:4] = jnp.sum(jnp.where(matches, logits, 0.0), axis=0, keepdims=True)
    stats[0] = own[...]

    def stat_copy(k):
        return pltpu.make_async_remote_copy(
            src_ref=own, dst_ref=stats.at[k], send_sem=ss.at[k], recv_sem=sr.at[k],
            device_id=at_offset(k), device_id_type=MESH
        )

    def tell(i, carry):
        stat_copy(1 + lax.rem(i + n // 4, n - 1)).start()
        return carry

    def hear(k, carry):
        stat_copy(k).wait()
        return carry

    lax.fori_loop(1, n, tell, 0)
    lax.fori_loop(1, n, hear, 0)
    every = stats[...]
    top = jnp.max(every[:, 0:1, :], axis=0)
    total = jnp.sum(every * jnp.exp(every[:, 0:1, :] - top[None]), axis=0)
    target = jnp.sum(every[:, 3:4, :], axis=0)
    sumexp, moment = total[1:2], total[2:3]
    lse = top + jnp.log(sumexp)
    mean_logit = moment / sumexp
    ratio = jnp.exp(target - lse - old)
    clipped = ((advant > 0.0) & (ratio > 1.2)) | ((advant < 0.0) & (ratio < 0.8))
    active = jnp.where(clipped, 0.0, 1.0)
    policy = -advant * ratio * active * weights
    logits = logit[...]
    probability = jnp.exp(logits - lse)
    onehot = jnp.where(matches, 1.0, 0.0)
    dt = policy * (onehot - probability) + 0.05 * weights * probability * (logits - mean_logit)
    dt_ref[...] = dt.astype(BF16)
    d = dt.T.astype(BF16)

    def weigh(p):
        begin, end = spans[p]
        cc = step_of(end - begin, 512)
        for at in range(begin, end, cc):
            rows = g[:, :, :, :, at:at + cc].reshape(T, cc)
            gw_ref[:, at:at + cc] = jnp.dot(dt_ref[...], rows, preferred_element_type=F32).astype(BF16)

    halves, line = [[] for _ in range(parts)], [[] for _ in range(parts)]
    first, second = [[] for _ in range(parts)], [[] for _ in range(parts)]
    for p, s in waves(parts, SCATTER_DELAYS):
        a, b = mine[p]
        cols = gcuts[p]
        here = block(p, slice(None), b) + (slice(None), cols)
        if s == 0:
            begin, end = spans[p]
            cc = step_of(end - begin, 512)
            for at in range(begin, end, cc):
                piece = jnp.dot(d, wt[:, at:at + cc], preferred_element_type=F32)
                pb[:, :, :, :, at:at + cc] = piece.reshape(C, X, Y, R, cc)
            halves[p] = [
                send(pb.at[lax.rem(c + k, C), :, :, :, cols], rc.at[k - 1, :, :, :, cols],
                     ks.at[p, k], kr.at[p, k], device(z, y, x, lax.rem(c + k, C)))
                for k in range(1, C)
            ]
        elif s == 1:
            for copy in halves[p]:
                copy.wait_recv()
            acc = pb[c, :, :, :, cols]
            for k in range(1, C):
                acc = acc + rc[k - 1, :, :, :, cols]
            pb[c, :, :, :, cols] = acc
            sb[:, :, :, cols] = acc.astype(BF16)
            for k in range(1, sizes[p][1]):
                other = lax.rem(b + k, sizes[p][1])
                second[p].append(send(sb.at[block(p, slice(None), other) + (slice(None), cols)],
                                      lands[2 * p].at[k - 1], t1s.at[p, k], t1r.at[p, k], plane_device(p, 0, k)))
        elif s == 2:
            for copy in second[p]:
                copy.wait_recv()
            acc = pb[(c,) + here]
            for k in range(1, sizes[p][1]):
                acc = acc + lands[2 * p][k - 1].astype(F32)
            pb[(c,) + here] = acc
            sb[here] = acc.astype(BF16)
            for k in range(1, sizes[p][0]):
                other = lax.rem(a + k, sizes[p][0])
                first[p].append(send(sb.at[block(p, other, b) + (slice(None), cols)],
                                     lands[2 * p + 1].at[k - 1], t2s.at[p, k], t2r.at[p, k], plane_device(p, k, 0)))
        elif s == 3:
            for copy in first[p]:
                copy.wait_recv()
            acc = pb[c, x, y, :, cols]
            for k in range(1, sizes[p][0]):
                acc = acc + lands[2 * p + 1][k - 1].astype(F32)
            stage[:, cols] = acc
            for zi in range(Z):
                piece = stage[zi * rp:(zi + 1) * rp, cols]
                qf[zi, :, cols] = piece
                q[zi, :, cols] = piece.astype(BF16)
            line[p] = [
                send(q.at[lax.rem(z + k, Z), :, cols], rz.at[k, :, cols], us.at[p, k], ur.at[p, k],
                     device(lax.rem(z + k, Z), y, x, c))
                for k in range(1, Z)
            ]
        else:
            acc = qf[z, :, cols]
            for k in range(1, Z):
                line[p][k - 1].wait_recv()
                acc = acc + rz[k, :, cols].astype(F32)
            gh_ref[:, cols] = acc[0:real]
        if (p, s) == (parts - 1, 1):
            for other in range(parts // 2):
                weigh(other)
        if (p, s) == (parts - 1, 2):
            for other in range(parts // 2, parts):
                weigh(other)
    for copy in started:
        copy.wait_send()


def per_device(dims, hidden, head_weight, actions, old_logp, advantage, loss_mask):
    Z, Y, X, C = dims
    n = Z * Y * X * C
    real, D = hidden.shape
    width = head_weight.shape[1]
    rp = real
    while Z * rp % 16:
        rp += 1
    R, T = Z * rp, n * rp
    parts = PARTS
    spans = part_columns(D, parts)
    vmem = pl.BlockSpec(memory_space=pltpu.VMEM)
    hbm = pl.BlockSpec(memory_space=pltpu.HBM)
    dma = pltpu.SemaphoreType.DMA
    most = max(X, Y, Z, C)
    shared = max((C - 1) * (X + Y - 1), 1)
    lands = []
    for p, (begin, end) in enumerate(spans):
        one, two = (Y, X) if p % 2 == 0 else (X, Y)
        lands.append(pltpu.VMEM((max(two - 1, 1), one, R, end - begin), BF16))
        lands.append(pltpu.VMEM((max(one - 1, 1), R, end - begin), BF16))
    buffers = [
        pltpu.VMEM((width, D), BF16),
        pltpu.VMEM((width, T), BF16),
        pltpu.VMEM((rp, D + LANES), BF16),
        pltpu.VMEM((Z, rp, D + LANES), BF16),
        pltpu.VMEM((R, D + LANES), F32),
        pltpu.VMEM((C, X, Y, R, D + LANES), BF16),
        pltpu.VMEM((4, T), F32),
        pltpu.VMEM((n, 4, T), F32),
        pltpu.VMEM((width, T), F32),
        pltpu.VMEM((C, X, Y, R, D), F32),
        pltpu.VMEM((max(C - 1, 1), X, Y, R, D), F32),
        pltpu.VMEM((X, Y, R, D), BF16),
        pltpu.VMEM((Z, rp, D), BF16),
        pltpu.VMEM((Z, rp, D), F32),
        pltpu.VMEM((Z, rp, D), BF16),
    ]
    taken = sum(math.prod(b.shape) * b.dtype.itemsize for b in buffers + lands) + 2 * width * D
    grant = min(taken * 5 // 4 + (8 << 20), 60 * 1024 * 1024)
    grad_hidden, grad_weight = pl.pallas_call(
        functools.partial(kernel, dims, real, parts),
        out_shape=(
            jax.ShapeDtypeStruct((real, D), F32),
            jax.ShapeDtypeStruct((width, D), BF16),
        ),
        in_specs=[hbm] * 6,
        out_specs=(vmem, vmem),
        scratch_shapes=[
            pltpu.VMEM(hidden.shape, BF16),
            pltpu.SMEM(actions.shape, jnp.int32),
            pltpu.SMEM(loss_mask.shape, jnp.int32),
            pltpu.VMEM(old_logp.shape, BF16),
            pltpu.VMEM(advantage.shape, BF16),
            *buffers,
            dma((5,)),
            dma,
            dma((parts, Z)), dma((parts, Z)),
            dma((parts, most)), dma((parts, most)),
            dma((parts, most)), dma((parts, most)),
            dma((parts, shared)), dma((parts, shared)),
            dma((n,)), dma((n,)),
            dma((parts, most)), dma((parts, most)),
            dma((parts, most)), dma((parts, most)),
            dma((parts, most)), dma((parts, most)),
            dma((parts, Z)), dma((parts, Z)),
            *lands,
        ],
        compiler_params=pltpu.CompilerParams(
            collective_id=0, has_side_effects=True, vmem_limit_bytes=grant
        ),
    )(*(pltpu.with_memory_space_constraint(v, pltpu.HBM)
        for v in (hidden, actions, loss_mask, old_logp, advantage, head_weight.T)))
    return (grad_weight.T, grad_hidden)


def solution(mesh):
    tok, voc = mesh.shape["tok"], mesh.shape["voc"]
    inner = 2 if tok % 2 == 0 else 1
    cores = 2 if voc % 2 == 0 else 1
    dims = (tok // inner, inner, voc // cores, cores)
    placed = (
        P(("tok", "voc"), None),
        P(None, ("tok", "voc")),
        P(("tok", "voc")),
        P(("tok", "voc")),
        P(("tok", "voc")),
        P(("tok", "voc")),
    )
    return jax.shard_map(
        functools.partial(per_device, dims),
        mesh=mesh,
        in_specs=placed,
        out_specs=(P(None, ("tok", "voc")), P(("tok", "voc"), None)),
        check_vma=False,
    )
```
